64 devices in a mesh: dp: 4 (over x, y), tp: 16 (over z, core).
Axes of the slice: x: 2, y: 2, z: 8, core: 2. Of those that a mesh axis runs over, the one named last changes fastest.
The devices are a block of a 4x4x8 slice.
Arguments:
- x: bfloat16 [2048, 3072], P(('dp', 'tp')), parts along dimension 0
- dy: bfloat16 [2048, 3072], P(('dp', 'tp')), parts along dimension 0
- wg: bfloat16 [3072, 8192], P(None, 'tp')
- wu: bfloat16 [3072, 8192], P(None, 'tp')
- wd: bfloat16 [8192, 3072], P('tp')
Outputs:
- output 1: bfloat16 [2048, 3072], P(('dp', 'tp')), parts along dimension 0
- output 2: float32 [12288, 8192], P('dp', 'tp'), parts along dimension 0
- output 3: float32 [12288, 8192], P('dp', 'tp'), parts along dimension 0
- output 4: float32 [32768, 3072], P(('dp', 'tp')), parts along dimension 0
There are 4 independent parts. The reference program is written for one: setup_inputs(seed, part) draws one part's arguments, and reference() takes and returns one part's arrays. A program takes and returns all parts, laid end to end along the dimension named above; an argument that names none is the same for every part.
All inputs are finite; a program needn't handle non-finite values.
Results may differ from the reference program's by a relative error of at most 0.016622.
Values are sent between devices in bfloat16 or wider.
A program may use at most 768 MiB of HBM per device.

```python
import jax
import jax.numpy as jnp

T = 512
H = 3072
F = 8192


def setup_inputs(seed: int = 0, part: int = 0) -> dict:
    key = jax.random.PRNGKey(seed)
    kx, kdy = jax.random.split(jax.random.fold_in(key, part))
    kg, ku, kd = jax.random.split(key, 3)
    x = jax.random.normal(kx, (T, H), jnp.float32)
    dy = jax.random.normal(kdy, (T, H), jnp.float32)
    wg = jax.random.normal(kg, (H, F), jnp.float32) * H ** -0.5
    wu = jax.random.normal(ku, (H, F), jnp.float32) * H ** -0.5
    wd = jax.random.normal(kd, (F, H), jnp.float32) * F ** -0.5
    return {"x": x.astype(jnp.bfloat16), "dy": dy.astype(jnp.bfloat16),
            "wg": wg.astype(jnp.bfloat16), "wu": wu.astype(jnp.bfloat16),
            "wd": wd.astype(jnp.bfloat16)}


def _silu_and_grad(u):
    s = jax.nn.sigmoid(u)
    return u * s, s * (1.0 + u * (1.0 - s))


def reference(x, dy, wg, wu, wd):
    ug = jnp.dot(x, wg, preferred_element_type=jnp.float32).astype(jnp.bfloat16).astype(jnp.float32)
    uu = jnp.dot(x, wu, preferred_element_type=jnp.float32).astype(jnp.bfloat16).astype(jnp.float32)
    a, da = _silu_and_grad(ug)
    z = (a * uu).astype(jnp.bfloat16)
    dwd = jnp.dot(z.T, dy, preferred_element_type=jnp.float32)
    g = jnp.dot(dy, wd.T, preferred_element_type=jnp.float32)
    duu = (g * a).astype(jnp.bfloat16)
    dug = (g * uu * da).astype(jnp.bfloat16)
    p = jnp.dot(dug, wg.T, preferred_element_type=jnp.float32) + jnp.dot(duu, wu.T, preferred_element_type=jnp.float32)
    dx = p.astype(jnp.bfloat16)
    dwg = jnp.dot(x.T, dug, preferred_element_type=jnp.float32)
    dwu = jnp.dot(x.T, duu, preferred_element_type=jnp.float32)
    return dx, dwg, dwu, dwd
```

```python
import functools

import jax
import jax.numpy as jnp
from jax import lax
from jax.experimental import pallas as pl
from jax.experimental.pallas import tpu as pltpu
from jax.sharding import PartitionSpec as P

MESH = pl.DeviceIdType.MESH
F32 = jnp.float32
BF16 = jnp.bfloat16
CORES = 2
PIECES = 4
NT = (((1,), (1,)), ((), ()))


def _silu_and_grad(u):
    s = jax.nn.sigmoid(u)
    return u * s, s * (1.0 + u * (1.0 - s))


def _main_kernel(nz, rows, x_hbm, dy_hbm, wg_hbm, wu_hbm, wd_hbm,
                 dx_ref, xg_out, dyg_out, dug_out, duu_out, z_out,
                 xg, dyg, wg, wu, wd, dug, duu, zz, pown, psend, psib, rsend, rrecv,
                 own_sem, w_sem, ag_send, ag_recv, sib_send, sib_recv, ps_send, ps_recv,
                 rs_send, rs_recv, out_sem):
    far = nz // 2
    near = nz - 1 - far
    me = lax.axis_index("tp")
    z = me // CORES
    c = lax.rem(me, CORES)
    right = {"tp": lax.rem(z + 1, nz) * CORES + c}
    left = {"tp": lax.rem(z + nz - 1, nz) * CORES + c}
    sib = {"tp": z * CORES + (1 - c)}
    width = x_hbm.shape[1]
    pw = width // PIECES
    arrays = (xg, dyg)

    def chip(off):
        return lax.rem(z + off + 2 * nz, nz)

    own = [pltpu.make_async_copy(src, dst.at[z, 0], own_sem.at[i])
           for i, (src, dst) in enumerate(((x_hbm, xg), (dy_hbm, dyg)))]
    wcopies = [pltpu.make_async_copy(src, dst, w_sem.at[i])
               for i, (src, dst) in enumerate(((wg_hbm, wg), (wu_hbm, wu), (wd_hbm, wd)))]
    for cp in own:
        cp.start()
    for cp in wcopies:
        cp.start()
    barrier = pltpu.get_barrier_semaphore()
    for dev in (left, right, sib):
        pl.semaphore_signal(barrier, inc=1, device_id=dev, device_id_type=MESH)
    pl.semaphore_wait(barrier, 3)

    def ag_copy(a, d, s):
        src_chip = chip(1 - s) if d == 0 else chip(s - 1)
        blk = arrays[a].at[src_chip, 0]
        return pltpu.make_async_remote_copy(
            blk, blk, ag_send.at[a, d, s - 1], ag_recv.at[a, d, s - 1],
            device_id=right if d == 0 else left, device_id_type=MESH)

    def sib_copy(a, b):
        return pltpu.make_async_remote_copy(
            arrays[a].at[b, 0], arrays[a].at[b, 1], sib_send.at[a, b], sib_recv.at[a, b],
            device_id=sib, device_id_type=MESH)

    def psum_copy(b):
        return pltpu.make_async_remote_copy(
            psend.at[b], psib.at[b], ps_send.at[b], ps_recv.at[b], device_id=sib, device_id_type=MESH)

    def compute(b):
        for a in range(2):
            sib_copy(a, b).wait_recv()
        xb = xg[b].reshape(CORES * rows, width)
        dyb = dyg[b].reshape(CORES * rows, width)
        ug = jnp.dot(xb, wg[...], preferred_element_type=F32).astype(BF16).astype(F32)
        uu = jnp.dot(xb, wu[...], preferred_element_type=F32).astype(BF16).astype(F32)
        g = lax.dot_general(dyb, wd[...], NT, preferred_element_type=F32)
        a, da = _silu_and_grad(ug)
        zz[b] = (a * uu).astype(BF16)
        u = (g * a).astype(BF16)
        duu[b] = u
        v = (g * uu * da).astype(BF16)
        dug[b] = v
        for q in range(PIECES):
            cols = slice(q * pw, (q + 1) * pw)
            p = (lax.dot_general(v, wg[cols, :], NT, preferred_element_type=F32)
                 + lax.dot_general(u, wu[cols, :], NT, preferred_element_type=F32))
            pown[b, q] = p[:rows]
            psend[b, q] = p[rows:].astype(BF16)
        psum_copy(b).start()

    for a in range(2):
        own[a].wait()
        d0 = a
        ag_copy(a, d0, 1).start()
    for a in range(2):
        ag_copy(a, 1 - a, 1).start()
        sib_copy(a, z).start()
    for cp in wcopies:
        cp.wait()

    @pl.loop(1, far + 1)
    def _(s):
        for a in range(2):
            ag_copy(a, a, s).wait_recv()

            @pl.when(s < far)
            def _():
                ag_copy(a, a, s + 1).start()
            sib_copy(a, chip(-s) if a == 0 else chip(s)).start()
        compute(chip(s - 1))

        @pl.when(s <= near)
        def _():
            for a in range(2):
                ag_copy(a, 1 - a, s).wait_recv()

                @pl.when(s < near)
                def _():
                    ag_copy(a, 1 - a, s + 1).start()
                sib_copy(a, chip(s) if a == 0 else chip(-s)).start()
        compute(chip(-s))

    outs = [pltpu.make_async_copy(src, dst, out_sem.at[i]) for i, (src, dst) in enumerate(
        ((xg, xg_out), (dyg, dyg_out), (dug, dug_out), (duu, duu_out), (zz, z_out)))]
    for cp in outs:
        cp.start()

    def hops(d, q):
        return far if (q + d) % 2 == 0 else near

    def rs_copy(d, q, s):
        return pltpu.make_async_remote_copy(
            rsend.at[d, q, s], rrecv.at[d, q, s], rs_send.at[d, q, s], rs_recv.at[d, q, s],
            device_id=right if d == 0 else left, device_id_type=MESH)

    def partial(b, q):
        return pown[b, q] + psib[b, q].astype(F32)

    def rs_step(d, q, s):
        h = hops(d, q)
        b = chip(h - s) if d == 0 else chip(s - h)
        t = partial(b, q)
        if s > 0:
            rs_copy(d, q, s - 1).wait_recv()
            t = t + rrecv[d, q, s - 1].astype(F32)
        rsend[d, q, s] = t.astype(BF16)
        rs_copy(d, q, s).start()

    for off in range(nz):
        psum_copy(chip(off)).wait_recv()
    for s in range(far):
        for long in (False, True):
            for q in range(PIECES):
                for d in range(2):
                    if ((q + d) % 2 == 0) == long and s < hops(d, q):
                        rs_step(d, q, s)
    for q in range(PIECES):
        t = partial(z, q)
        for d in range(2):
            h = hops(d, q)
            rs_copy(d, q, h - 1).wait_recv()
            t = t + rrecv[d, q, h - 1].astype(F32)
        dx_ref[:, q * pw:(q + 1) * pw] = t.astype(BF16)

    for a in range(2):
        for d in range(2):
            for s in range(1, (far if a == d else near) + 1):
                ag_copy(a, d, s).wait_send()
        for off in range(nz):
            sib_copy(a, chip(off)).wait_send()
    for off in range(nz):
        psum_copy(chip(off)).wait_send()
    for d in range(2):
        for q in range(PIECES):
            for s in range(hops(d, q)):
                rs_copy(d, q, s).wait_send()
    for cp in outs:
        cp.wait()


def _grad_kernel(x_ref, dy_ref, dug_ref, duu_ref, z_ref, dwg_ref, dwu_ref, dwd_ref, zt):
    @pl.when(pl.program_id(0) == 0)
    def _():
        zt[...] = z_ref[...].T
    xt = x_ref[...].T
    dwg_ref[...] = jnp.dot(xt, dug_ref[...], preferred_element_type=F32)
    dwu_ref[...] = jnp.dot(xt, duu_ref[...], preferred_element_type=F32)
    dwd_ref[...] = jnp.dot(zt[...], dy_ref[...], preferred_element_type=F32)


def solution(mesh):
    n = mesh.shape["tp"]
    nz = n // CORES

    def local(x, dy, wg, wu, wd):
        rows, width = x.shape
        hid = wg.shape[1]
        tok = rows * n
        far = nz // 2
        pw = width // PIECES
        S = jax.ShapeDtypeStruct
        hbm = pl.BlockSpec(memory_space=pltpu.HBM)
        dma = pltpu.SemaphoreType.DMA
        dx, xg, dyg, dug, duu, z = pl.pallas_call(
            functools.partial(_main_kernel, nz, rows),
            out_shape=[S((rows, width), BF16)] + [S((nz, CORES, rows, width), BF16)] * 2
            + [S((nz, CORES * rows, hid), BF16)] * 3,
            in_specs=[hbm] * 5,
            out_specs=[pl.BlockSpec(memory_space=pltpu.VMEM)] + [hbm] * 5,
            scratch_shapes=[
                pltpu.VMEM((nz, CORES, rows, width), BF16),
                pltpu.VMEM((nz, CORES, rows, width), BF16),
                pltpu.VMEM((width, hid), BF16),
                pltpu.VMEM((width, hid), BF16),
                pltpu.VMEM((hid, width), BF16),
                pltpu.VMEM((nz, CORES * rows, hid), BF16),
                pltpu.VMEM((nz, CORES * rows, hid), BF16),
                pltpu.VMEM((nz, CORES * rows, hid), BF16),
                pltpu.VMEM((nz, PIECES, rows, pw), F32),
                pltpu.VMEM((nz, PIECES, rows, pw), BF16),
                pltpu.VMEM((nz, PIECES, rows, pw), BF16),
                pltpu.VMEM((2, PIECES, far, rows, pw), BF16),
                pltpu.VMEM((2, PIECES, far, rows, pw), BF16),
                dma((2,)), dma((3,)),
                dma((2, 2, far)), dma((2, 2, far)),
                dma((2, nz)), dma((2, nz)),
                dma((nz,)), dma((nz,)),
                dma((2, PIECES, far)), dma((2, PIECES, far)),
                dma((5,)),
            ],
            compiler_params=pltpu.CompilerParams(
                collective_id=0, has_side_effects=True, vmem_limit_bytes=56 * 1024 * 1024),
            cost_estimate=pl.CostEstimate(
                flops=2 * 5 * tok * width * hid, bytes_accessed=6 * width * hid, transcendentals=tok * hid),
            name="gather_compute_scatter",
        )(x, dy, wg, wu, wd)
        bw = 256
        whole = lambda i: (0, 0)
        dwg, dwu, dwd = pl.pallas_call(
            _grad_kernel,
            grid=(width // bw,),
            out_shape=[S((width, hid), F32), S((width, hid), F32), S((hid, width), F32)],
            in_specs=[pl.BlockSpec((tok, bw), lambda i: (0, i)), pl.BlockSpec((tok, bw), lambda i: (0, i)),
                      pl.BlockSpec((tok, hid), whole), pl.BlockSpec((tok, hid), whole),
                      pl.BlockSpec((tok, hid), whole)],
            out_specs=[pl.BlockSpec((bw, hid), lambda i: (i, 0)), pl.BlockSpec((bw, hid), lambda i: (i, 0)),
                       pl.BlockSpec((hid, bw), lambda i: (0, i))],
            scratch_shapes=[pltpu.VMEM((hid, tok), BF16)],
            compiler_params=pltpu.CompilerParams(vmem_limit_bytes=60 * 1024 * 1024),
            cost_estimate=pl.CostEstimate(
                flops=2 * 3 * tok * width * hid, bytes_accessed=12 * width * hid + 4 * tok * width, transcendentals=0),
            name="weight_grads",
        )(xg.reshape(tok, width), dyg.reshape(tok, width), dug.reshape(tok, hid), duu.reshape(tok, hid),
          z.reshape(tok, hid))
        return dx, dwg, dwu, dwd

    rows = P(("dp", "tp"), None)
    return jax.shard_map(local, mesh=mesh,
                         in_specs=(rows, rows, P(None, "tp"), P(None, "tp"), P("tp", None)),
                         out_specs=(rows, P("dp", "tp"), P("dp", "tp"), rows),
                         check_vma=False)
```

```python
import functools

import jax
import jax.numpy as jnp
from jax import lax
from jax.experimental import pallas as pl
from jax.experimental.pallas import tpu as pltpu
from jax.sharding import PartitionSpec as P

MESH = pl.DeviceIdType.MESH
F32 = jnp.float32
BF16 = jnp.bfloat16
CORES = 2
PIECES = 4
NT = (((1,), (1,)), ((), ()))


def _silu_and_grad(u):
    s = jax.nn.sigmoid(u)
    return u * s, s * (1.0 + u * (1.0 - s))


def _main_kernel(nz, rows, x_hbm, dy_hbm, wg_hbm, wu_hbm, wd_hbm,
                 dx_ref, xg, dug, dwu_ref, dwd_ref,
                 dyg, duu, zz, zt, wg, wu, wd, wgt, wut, wdt, pown, psend, psib, rsend, rrecv,
                 own_sem, w_sem, ag_send, ag_recv, sib_send, sib_recv, ps_send, ps_recv,
                 rs_send, rs_recv):
    far = nz // 2
    near = nz - 1 - far
    me = lax.axis_index("tp")
    z = me // CORES
    c = lax.rem(me, CORES)
    right = {"tp": lax.rem(z + 1, nz) * CORES + c}
    left = {"tp": lax.rem(z + nz - 1, nz) * CORES + c}
    sib = {"tp": z * CORES + (1 - c)}
    width = x_hbm.shape[1]
    pw = width // PIECES
    blk = CORES * rows
    arrays = (xg, dyg)

    def chip(off):
        return lax.rem(z + off + 2 * nz, nz)

    own = [pltpu.make_async_copy(src, dst.at[z, 0], own_sem.at[i])
           for i, (src, dst) in enumerate(((x_hbm, xg), (dy_hbm, dyg)))]
    wcopies = [pltpu.make_async_copy(src, dst, w_sem.at[i])
               for i, (src, dst) in enumerate(((wg_hbm, wg), (wu_hbm, wu), (wd_hbm, wd)))]
    for cp in own:
        cp.start()
    for cp in wcopies:
        cp.start()
    barrier = pltpu.get_barrier_semaphore()
    for dev in (left, right, sib):
        pl.semaphore_signal(barrier, inc=1, device_id=dev, device_id_type=MESH)
    pl.semaphore_wait(barrier, 3)

    def ag_copy(a, d, s):
        src_chip = chip(1 - s) if d == 0 else chip(s - 1)
        part = arrays[a].at[src_chip, 0]
        return pltpu.make_async_remote_copy(
            part, part, ag_send.at[a, d, s - 1], ag_recv.at[a, d, s - 1],
            device_id=right if d == 0 else left, device_id_type=MESH)

    def sib_copy(a, b):
        return pltpu.make_async_remote_copy(
            arrays[a].at[b, 0], arrays[a].at[b, 1], sib_send.at[a, b], sib_recv.at[a, b],
            device_id=sib, device_id_type=MESH)

    def psum_copy(b, q):
        return pltpu.make_async_remote_copy(
            psend.at[b, q], psib.at[b, q], ps_send.at[b, q], ps_recv.at[b, q], device_id=sib, device_id_type=MESH)

    def stack(parts):
        return parts[0] if len(parts) == 1 else jnp.concatenate(parts, axis=0)

    def compute(bs):
        for b in bs:
            for a in range(2):
                sib_copy(a, b).wait_recv()
        xb = stack([xg[b].reshape(blk, width) for b in bs])
        dyb = stack([dyg[b].reshape(blk, width) for b in bs])
        ug = jnp.dot(xb, wg[...], preferred_element_type=F32).astype(BF16).astype(F32)
        uu = jnp.dot(xb, wu[...], preferred_element_type=F32).astype(BF16).astype(F32)
        g = jnp.dot(dyb, wdt[...], preferred_element_type=F32)
        a, da = _silu_and_grad(ug)
        zv = (a * uu).astype(BF16)
        u = (g * a).astype(BF16)
        v = (g * uu * da).astype(BF16)
        for i, b in enumerate(bs):
            part = slice(i * blk, (i + 1) * blk)
            zz[b] = zv[part]
            duu[b] = u[part]
            dug[b] = v[part]
        for q in range(PIECES):
            cols = slice(q * pw, (q + 1) * pw)
            p = (jnp.dot(v, wgt[:, cols], preferred_element_type=F32)
                 + jnp.dot(u, wut[:, cols], preferred_element_type=F32))
            for i, b in enumerate(bs):
                pown[b, q] = p[i * blk:i * blk + rows]
                psend[b, q] = p[i * blk + rows:(i + 1) * blk].astype(BF16)
                psum_copy(b, q).start()

    def hops(d, q):
        return far if (q + d) % 2 == 0 else near

    def rs_copy(d, q, s):
        return pltpu.make_async_remote_copy(
            rsend.at[d, q, s], rrecv.at[d, q, s], rs_send.at[d, q, s], rs_recv.at[d, q, s],
            device_id=right if d == 0 else left, device_id_type=MESH)

    def partial(b, q):
        psum_copy(b, q).wait_recv()
        return pown[b, q] + psib[b, q].astype(F32)

    def rs_round(s, h):
        for q in range(PIECES):
            for d in range(2):
                if hops(d, q) == h and s < h:
                    t = partial(chip(h - s) if d == 0 else chip(s - h), q)
                    if s > 0:
                        rs_copy(d, q, s - 1).wait_recv()
                        t = t + rrecv[d, q, s - 1].astype(F32)
                    rsend[d, q, s] = t.astype(BF16)
                    rs_copy(d, q, s).start()

    def grad_chunk(i, n):
        tok, w = nz * blk, width // n
        part = slice(i * w, (i + 1) * w)
        if i == 0:
            zt[...] = zz[...].reshape(tok, zz.shape[2]).T
        dwd_ref[:, part] = jnp.dot(zt[...], dyg[:, :, :, part].reshape(tok, w), preferred_element_type=F32)
        xt = xg[:, :, :, part].reshape(tok, w).T
        dwu_ref[part, :] = jnp.dot(xt, duu[...].reshape(tok, duu.shape[2]), preferred_element_type=F32)

    for a in range(2):
        own[a].wait()
        ag_copy(a, a, 1).start()
    for a in range(2):
        ag_copy(a, 1 - a, 1).start()
        sib_copy(a, z).start()
    for cp, w, wt in zip(wcopies, (wg, wu, wd), (wgt, wut, wdt)):
        cp.wait()
        wt[...] = w[...].T
    compute([z])

    def first_arrivals(s, forward):
        for a in range(2):
            ag_copy(a, a, s).wait_recv()
            if forward:
                ag_copy(a, a, s + 1).start()
            sib_copy(a, chip(-s) if a == 0 else chip(s)).start()

    @pl.loop(1, near + 1)
    def _(s):
        first_arrivals(s, True)
        for a in range(2):
            ag_copy(a, 1 - a, s).wait_recv()

            @pl.when(s < near)
            def _():
                ag_copy(a, 1 - a, s + 1).start()
            sib_copy(a, chip(s) if a == 0 else chip(-s)).start()
        compute([chip(s), chip(-s)])

    first_arrivals(far, False)
    rs_round(0, near)
    compute([chip(far)])
    for s in range(1, far + 1):
        rs_round(s - 1, far)
        rs_round(s, near)
        if s < far:
            grad_chunk(s - 1, far - 1)
    for q in range(PIECES):
        t = partial(z, q)
        for d in range(2):
            h = hops(d, q)
            rs_copy(d, q, h - 1).wait_recv()
            t = t + rrecv[d, q, h - 1].astype(F32)
        dx_ref[:, q * pw:(q + 1) * pw] = t.astype(BF16)

    for a in range(2):
        for d in range(2):
            for s in range(1, (far if a == d else near) + 1):
                ag_copy(a, d, s).wait_send()
        for off in range(nz):
            sib_copy(a, chip(off)).wait_send()
    for off in range(nz):
        for q in range(PIECES):
            psum_copy(chip(off), q).wait_send()
    for d in range(2):
        for q in range(PIECES):
            for s in range(hops(d, q)):
                rs_copy(d, q, s).wait_send()


def _grad_kernel(bw, x_ref, dug_ref, dx_vmem, dwu_vmem, dwd_vmem, dx_ref, dwg_ref, dwu_ref, dwd_ref, buf, done_sem, sem):
    steps = x_ref.shape[1] // bw
    stores = [pltpu.make_async_copy(src, dst, done_sem.at[i]) for i, (src, dst) in enumerate(
        ((dwd_vmem, dwd_ref), (dwu_vmem, dwu_ref), (dx_vmem, dx_ref)))]
    for cp in stores:
        cp.start()
    for i in range(steps):
        part = slice(i * bw, (i + 1) * bw)
        buf[part] = jnp.dot(x_ref[:, part].T, dug_ref[...], preferred_element_type=F32)
        stores.append(pltpu.make_async_copy(buf.at[part], dwg_ref.at[part], sem.at[i]))
        stores[-1].start()
    for cp in stores:
        cp.wait()


def solution(mesh):
    n = mesh.shape["tp"]
    nz = n // CORES

    def local(x, dy, wg, wu, wd):
        x, dy, wg, wu, wd = (pltpu.with_memory_space_constraint(v, pltpu.HBM) for v in (x, dy, wg, wu, wd))
        rows, width = x.shape
        hid = wg.shape[1]
        tok = rows * n
        far = nz // 2
        pw = width // PIECES
        S = jax.ShapeDtypeStruct
        hbm = pl.BlockSpec(memory_space=pltpu.HBM)
        dma = pltpu.SemaphoreType.DMA
        vmem = pl.BlockSpec(memory_space=pltpu.VMEM)
        dx, xg, dug, dwu, dwd = pl.pallas_call(
            functools.partial(_main_kernel, nz, rows),
            out_shape=[S((rows, width), BF16), S((nz, CORES, rows, width), BF16),
                       S((nz, CORES * rows, hid), BF16), S((width, hid), F32), S((hid, width), F32)],
            in_specs=[hbm] * 5,
            out_specs=[vmem] * 5,
            scratch_shapes=[
                pltpu.VMEM((nz, CORES, rows, width), BF16),
                pltpu.VMEM((nz, CORES * rows, hid), BF16),
                pltpu.VMEM((nz, CORES * rows, hid), BF16),
                pltpu.VMEM((hid, tok), BF16),
                pltpu.VMEM((width, hid), BF16),
                pltpu.VMEM((width, hid), BF16),
                pltpu.VMEM((hid, width), BF16),
                pltpu.VMEM((hid, width), BF16),
                pltpu.VMEM((hid, width), BF16),
                pltpu.VMEM((width, hid), BF16),
                pltpu.VMEM((nz, PIECES, rows, pw), F32),
                pltpu.VMEM((nz, PIECES, rows, pw), BF16),
                pltpu.VMEM((nz, PIECES, rows, pw), BF16),
                pltpu.VMEM((2, PIECES, far, rows, pw), BF16),
                pltpu.VMEM((2, PIECES, far, rows, pw), BF16),
                dma((2,)), dma((3,)),
                dma((2, 2, far)), dma((2, 2, far)),
                dma((2, nz)), dma((2, nz)),
                dma((nz, PIECES)), dma((nz, PIECES)),
                dma((2, PIECES, far)), dma((2, PIECES, far)),
            ],
            compiler_params=pltpu.CompilerParams(
                collective_id=0, has_side_effects=True, vmem_limit_bytes=36 * 1024 * 1024),
            cost_estimate=pl.CostEstimate(
                flops=2 * 5 * tok * width * hid, bytes_accessed=6 * width * hid, transcendentals=tok * hid),
            name="gather_compute_scatter",
        )(x, dy, wg, wu, wd)
        bw = 512
        dx, dwg, dwu, dwd = pl.pallas_call(
            functools.partial(_grad_kernel, bw),
            out_shape=[S((rows, width), BF16), S((width, hid), F32), S((width, hid), F32), S((hid, width), F32)],
            in_specs=[vmem] * 5,
            out_specs=[hbm] * 4,
            scratch_shapes=[pltpu.VMEM((width, hid), F32), dma((3,)), dma((width // bw,))],
            compiler_params=pltpu.CompilerParams(vmem_limit_bytes=16 * 1024 * 1024),
            cost_estimate=pl.CostEstimate(
                flops=2 * tok * width * hid, bytes_accessed=12 * width * hid, transcendentals=0),
            name="weight_grads",
        )(xg.reshape(tok, width), dug.reshape(tok, hid), dx, dwu, dwd)
        return dx, dwg, dwu, dwd

    rows = P(("dp", "tp"), None)
    return jax.shard_map(local, mesh=mesh,
                         in_specs=(rows, rows, P(None, "tp"), P(None, "tp"), P("tp", None)),
                         out_specs=(rows, P("dp", "tp"), P("dp", "tp"), rows),
                         check_vma=False)
```

```python
import functools

import jax
import jax.numpy as jnp
from jax import lax
from jax.experimental import pallas as pl
from jax.experimental.pallas import tpu as pltpu
from jax.sharding import PartitionSpec as P

MESH = pl.DeviceIdType.MESH
F32 = jnp.float32
BF16 = jnp.bfloat16
CORES = 2
PIECES = 4
NT = (((1,), (1,)), ((), ()))


def _silu_and_grad(u):
    s = jax.nn.sigmoid(u)
    return u * s, s * (1.0 + u * (1.0 - s))


def _main_kernel(nz, rows, x_hbm, dy_hbm, wg_hbm, wu_hbm, wd_hbm,
                 dx_ref, xg, dug, dwu_ref, dwd_ref,
                 dyg, duu, zz, zt, wg, wu, wd, wgt, wut, wdt,
                 pown, psend, psib, own_sum, own_send, own_sib, rsend, rrecv, fin,
                 own_sem, w_sem, ag_send, ag_recv, sib_send, sib_recv, ps_send, ps_recv, os_send, os_recv,
                 rs_send, rs_recv, fin_send, fin_recv):
    far = nz // 2
    near = nz - 1 - far
    me = lax.axis_index("tp")
    z = me // CORES
    c = lax.rem(me, CORES)
    width = x_hbm.shape[1]
    pw = width // PIECES
    blk = CORES * rows
    arrays = (xg, dyg)

    def dev(step, core):
        return {"tp": lax.rem(z + step + nz, nz) * CORES + core}

    def slot(off):
        return lax.rem(off + 2 * nz, nz)

    def step_of(d):
        return 1 if d == 0 else -1

    own = [pltpu.make_async_copy(src, dst.at[0, c], own_sem.at[i])
           for i, (src, dst) in enumerate(((x_hbm, xg), (dy_hbm, dyg)))]
    wcopies = [pltpu.make_async_copy(src, dst, w_sem.at[i])
               for i, (src, dst) in enumerate(((wg_hbm, wg), (wu_hbm, wu), (wd_hbm, wd)))]
    for cp in own:
        cp.start()
    for cp in wcopies:
        cp.start()
    barrier = pltpu.get_barrier_semaphore()
    peers = [dev(0, 1 - c), dev(1, c), dev(-1, c), dev(1, 1 - c), dev(-1, 1 - c)]
    for peer in peers:
        pl.semaphore_signal(barrier, inc=1, device_id=peer, device_id_type=MESH)
    pl.semaphore_wait(barrier, len(peers))

    def ag_copy(a, d, s):
        off = 1 - s if d == 0 else s - 1
        return pltpu.make_async_remote_copy(
            arrays[a].at[slot(off), c], arrays[a].at[slot(off - step_of(d)), c],
            ag_send.at[a, d, s - 1], ag_recv.at[a, d, s - 1], device_id=dev(step_of(d), c), device_id_type=MESH)

    def far_copy(a, d):
        off = 1 - far if d == 0 else far - 1
        cols = pl.ds(d * (width // 2), width // 2)
        return pltpu.make_async_remote_copy(
            arrays[a].at[slot(off), c, :, cols], arrays[a].at[far, c, :, cols],
            ag_send.at[a, d, far - 1], ag_recv.at[a, d, far - 1], device_id=dev(step_of(d), c), device_id_type=MESH)

    def sib_copy(a, o):
        return pltpu.make_async_remote_copy(
            arrays[a].at[o, c], arrays[a].at[o, c], sib_send.at[a, o], sib_recv.at[a, o],
            device_id=dev(0, 1 - c), device_id_type=MESH)

    def sib_wait(a, o):
        pltpu.make_async_remote_copy(
            arrays[a].at[o, 1 - c], arrays[a].at[o, 1 - c], sib_send.at[a, o], sib_recv.at[a, o],
            device_id=dev(0, 1 - c), device_id_type=MESH).wait_recv()

    FAR = "far"

    def kept(o, q):
        if o is FAR:
            return (far if q % 2 == 0 else 0), q // 2
        return o, q // 2

    def psum_copy(o, q):
        k = kept(o, q)
        return pltpu.make_async_remote_copy(
            psend.at[k], psib.at[k], ps_send.at[k], ps_recv.at[k], device_id=dev(0, 1 - c), device_id_type=MESH)

    def own_copy(q):
        return pltpu.make_async_remote_copy(
            own_send.at[q], own_sib.at[q], os_send.at[q], os_recv.at[q], device_id=dev(0, 1 - c), device_id_type=MESH)

    def stack(ref, offs):
        parts = [ref[o].reshape(blk, ref.shape[-1]) for o in offs]
        return parts[0] if len(parts) == 1 else jnp.concatenate(parts, axis=0)

    def unstack(ref, offs, v):
        for i, o in enumerate(offs):
            ref[o] = v[i * blk:(i + 1) * blk]

    def x_part(offs):
        for o in offs:
            sib_wait(0, o)
        xb = stack(xg, offs)
        unstack(dug, offs, jnp.dot(xb, wg[...], preferred_element_type=F32).astype(BF16))
        unstack(duu, offs, jnp.dot(xb, wu[...], preferred_element_type=F32).astype(BF16))

    def y_part(offs, kind):
        for o in offs:
            sib_wait(1, o)
        g = jnp.dot(stack(dyg, offs), wdt[...], preferred_element_type=F32)
        ug = stack(dug, offs).astype(F32)
        uu = stack(duu, offs).astype(F32)
        a, da = _silu_and_grad(ug)
        unstack(zz, offs, (a * uu).astype(BF16))
        u = (g * a).astype(BF16)
        v = (g * uu * da).astype(BF16)
        unstack(duu, offs, u)
        unstack(dug, offs, v)
        for q in range(PIECES):
            cols = slice(q * pw, (q + 1) * pw)
            p = (jnp.dot(v, wgt[:, cols], preferred_element_type=F32)
                 + jnp.dot(u, wut[:, cols], preferred_element_type=F32))
            if kind == "own":
                own_sum[q] = jnp.where(c == 0, p[:rows], p[rows:])
                own_send[q] = jnp.where(c == 0, p[rows:], p[:rows]).astype(BF16)
                own_copy(q).start()
            elif kind == "far":
                pown[kept(FAR, q)] = p
                psend[kept(FAR, q)] = p.astype(BF16)

                @pl.when(c == 0)
                def _():
                    psum_copy(FAR, q).start()
            else:
                first = c if q % 2 == 0 else 1 - c
                keep_o = offs[1] + first * (offs[0] - offs[1])
                send_o = offs[0] + offs[1] - keep_o
                pown[kept(keep_o, q)] = jnp.where(first == 1, p[:blk], p[blk:])
                psend[kept(send_o, q)] = jnp.where(first == 1, p[blk:], p[:blk]).astype(BF16)
                psum_copy(send_o, q).start()

    def hops(d, q):
        return far if (q + d) % 2 == 0 else near

    def rs_copy(d, q, s):
        k = (d, q // 2, s)
        return pltpu.make_async_remote_copy(
            rsend.at[k], rrecv.at[k], rs_send.at[k], rs_recv.at[k], device_id=dev(step_of(d), c), device_id_type=MESH)

    def fin_copy(d, q, h):
        return pltpu.make_async_remote_copy(
            rsend.at[d, q // 2, hops(d, q) - 1, pl.ds(h * rows, rows)], fin.at[d, q],
            fin_send.at[d, q // 2, h], fin_recv.at[d, q], device_id=dev(step_of(d), h), device_id_type=MESH)

    def rs_round(s, n):
        for q in range(PIECES):
            for d in range(2):
                if hops(d, q) != n:
                    continue
                o = (n - s if d == 0 else s - n) % nz
                o = FAR if o == far else o
                psum_copy(o, q).wait_recv()
                t = pown[kept(o, q)] + psib[kept(o, q)].astype(F32)
                if s > 0:
                    rs_copy(d, q, s - 1).wait_recv()
                    t = t + rrecv[d, q // 2, s - 1].astype(F32)
                rsend[d, q // 2, s] = t.astype(BF16)
                if s < n - 1:
                    rs_copy(d, q, s).start()
                else:
                    for h in range(CORES):
                        fin_copy(d, q, h).start()

    def rs_drain(n):
        for d in range(2):
            for q in range(PIECES):
                if hops(d, q) == n:
                    for s in range(n - 1):
                        rs_copy(d, q, s).wait_send()
                    for h in range(CORES):
                        fin_copy(d, q, h).wait_send()

    def grad_chunk(i, n):
        tok, w = nz * blk, width // n
        part = slice(i * w, (i + 1) * w)
        if i == 0:
            zt[...] = zz[...].reshape(tok, zz.shape[2]).T
        dwd_ref[:, part] = jnp.dot(zt[...], dyg[:, :, :, part].reshape(tok, w), preferred_element_type=F32)
        xt = xg[:, :, :, part].reshape(tok, w).T
        dwu_ref[part, :] = jnp.dot(xt, duu[...].reshape(tok, duu.shape[2]), preferred_element_type=F32)

    for a in range(2):
        own[a].wait()
        for d in range(2):
            ag_copy(a, d, 1).start()
        sib_copy(a, 0).start()
    for cp, w, wt in zip(wcopies, (wg, wu, wd), (wgt, wut, wdt)):
        cp.wait()
        wt[...] = w[...].T
    def event(a, s):
        for d in range(2):
            ag_copy(a, d, s).wait_recv()
            if isinstance(s, int):
                (ag_copy(a, d, s + 1) if s < near else far_copy(a, d)).start()
            else:
                @pl.when(s < near)
                def _():
                    ag_copy(a, d, s + 1).start()

                @pl.when(s == near)
                def _():
                    far_copy(a, d).start()
            sib_copy(a, nz - s if d == 0 else s).start()

    def far_event(a):
        for d in range(2):
            far_copy(a, d).wait_recv()
        sib_copy(a, far).start()

    x_part([0])
    event(0, 1)
    y_part([0], "own")
    event(1, 1)
    x_part([1, nz - 1])

    @pl.loop(2, near + 1)
    def _(s):
        event(0, s)
        y_part([s - 1, nz + 1 - s], "pair")
        event(1, s)
        x_part([s, nz - s])

    far_event(0)
    y_part([near, nz - near], "pair")
    far_event(1)

    x_part([far])

    @pl.when(c == 0)
    def _():
        rs_round(0, near)
    y_part([far], "far")

    @pl.when(c == 1)
    def _():
        for s in range(far):
            rs_round(s, far)
            if s < far - 1:
                grad_chunk(s, far - 1)
        rs_drain(far)

    @pl.when(c == 0)
    def _():
        for s in range(1, near):
            rs_round(s, near)
            grad_chunk(s - 1, near)
        grad_chunk(near - 1, near)
        rs_drain(near)

    for q in range(PIECES):
        own_copy(q).wait_recv()
        t = own_sum[q] + own_sib[q].astype(F32)
        for d in range(2):
            fin_copy(d, q, 0).wait_recv()
            t = t + fin[d, q].astype(F32)
        dx_ref[:, q * pw:(q + 1) * pw] = t.astype(BF16)

    for a in range(2):
        for d in range(2):
            for s in range(1, far):
                ag_copy(a, d, s).wait_send()
            far_copy(a, d).wait_send()
        for o in range(nz):
            sib_copy(a, o).wait_send()
    for q in range(PIECES):
        own_copy(q).wait_send()
    for o in range(1, nz):
        if o != far:
            for q in range(0, PIECES, 2):
                psum_copy(o, q).wait_send()

    @pl.when(c == 0)
    def _():
        for q in range(PIECES):
            psum_copy(FAR, q).wait_send()


def _grad_kernel(bw, x_ref, dug_ref, dx_vmem, dwu_vmem, dwd_vmem, dx_ref, dwg_ref, dwu_ref, dwd_ref, buf, done_sem, sem):
    steps = x_ref.shape[1] // bw
    stores = [pltpu.make_async_copy(src, dst, done_sem.at[i]) for i, (src, dst) in enumerate(
        ((dwd_vmem, dwd_ref), (dwu_vmem, dwu_ref), (dx_vmem, dx_ref)))]
    for cp in stores:
        cp.start()
    for i in range(steps):
        part = slice(i * bw, (i + 1) * bw)
        buf[part] = jnp.dot(x_ref[:, part].T, dug_ref[...], preferred_element_type=F32)
        stores.append(pltpu.make_async_copy(buf.at[part], dwg_ref.at[part], sem.at[i]))
        stores[-1].start()
    for cp in stores:
        cp.wait()


def solution(mesh):
    n = mesh.shape["tp"]
    nz = n // CORES

    def local(x, dy, wg, wu, wd):
        x, dy, wg, wu, wd = (pltpu.with_memory_space_constraint(v, pltpu.HBM) for v in (x, dy, wg, wu, wd))
        rows, width = x.shape
        hid = wg.shape[1]
        tok = rows * n
        far = nz // 2
        pw = width // PIECES
        S = jax.ShapeDtypeStruct
        hbm = pl.BlockSpec(memory_space=pltpu.HBM)
        dma = pltpu.SemaphoreType.DMA
        vmem = pl.BlockSpec(memory_space=pltpu.VMEM)
        dx, xg, dug, dwu, dwd = pl.pallas_call(
            functools.partial(_main_kernel, nz, rows),
            out_shape=[S((rows, width), BF16), S((nz, CORES, rows, width), BF16),
                       S((nz, CORES * rows, hid), BF16), S((width, hid), F32), S((hid, width), F32)],
            in_specs=[hbm] * 5,
            out_specs=[vmem] * 5,
            scratch_shapes=[
                pltpu.VMEM((nz, CORES, rows, width), BF16),
                pltpu.VMEM((nz, CORES * rows, hid), BF16),
                pltpu.VMEM((nz, CORES * rows, hid), BF16),
                pltpu.VMEM((hid, tok), BF16),
                pltpu.VMEM((width, hid), BF16),
                pltpu.VMEM((width, hid), BF16),
                pltpu.VMEM((hid, width), BF16),
                pltpu.VMEM((hid, width), BF16),
                pltpu.VMEM((hid, width), BF16),
                pltpu.VMEM((width, hid), BF16),
                pltpu.VMEM((nz, PIECES // 2, CORES * rows, pw), F32),
                pltpu.VMEM((nz, PIECES // 2, CORES * rows, pw), BF16),
                pltpu.VMEM((nz, PIECES // 2, CORES * rows, pw), BF16),
                pltpu.VMEM((PIECES, rows, pw), F32),
                pltpu.VMEM((PIECES, rows, pw), BF16),
                pltpu.VMEM((PIECES, rows, pw), BF16),
                pltpu.VMEM((2, PIECES // 2, far, CORES * rows, pw), BF16),
                pltpu.VMEM((2, PIECES // 2, far, CORES * rows, pw), BF16),
                pltpu.VMEM((2, PIECES, rows, pw), BF16),
                dma((2,)), dma((3,)),
                dma((2, 2, far)), dma((2, 2, far)),
                dma((2, nz)), dma((2, nz)),
                dma((nz, PIECES // 2)), dma((nz, PIECES // 2)),
                dma((PIECES,)), dma((PIECES,)),
                dma((2, PIECES // 2, far)), dma((2, PIECES // 2, far)),
                dma((2, PIECES // 2, CORES)), dma((2, PIECES)),
            ],
            compiler_params=pltpu.CompilerParams(
                collective_id=0, has_side_effects=True, vmem_limit_bytes=36 * 1024 * 1024),
            cost_estimate=pl.CostEstimate(
                flops=2 * 5 * tok * width * hid, bytes_accessed=6 * width * hid, transcendentals=tok * hid),
            name="gather_compute_scatter",
        )(x, dy, wg, wu, wd)
        bw = 512
        dx, dwg, dwu, dwd = pl.pallas_call(
            functools.partial(_grad_kernel, bw),
            out_shape=[S((rows, width), BF16), S((width, hid), F32), S((width, hid), F32), S((hid, width), F32)],
            in_specs=[vmem] * 5,
            out_specs=[hbm] * 4,
            scratch_shapes=[pltpu.VMEM((width, hid), F32), dma((3,)), dma((width // bw,))],
            compiler_params=pltpu.CompilerParams(vmem_limit_bytes=16 * 1024 * 1024),
            cost_estimate=pl.CostEstimate(
                flops=2 * tok * width * hid, bytes_accessed=12 * width * hid, transcendentals=0),
            name="weight_grads",
        )(xg.reshape(tok, width), dug.reshape(tok, hid), dx, dwu, dwd)
        return dx, dwg, dwu, dwd

    rows = P(("dp", "tp"), None)
    return jax.shard_map(local, mesh=mesh,
                         in_specs=(rows, rows, P(None, "tp"), P(None, "tp"), P("tp", None)),
                         out_specs=(rows, P("dp", "tp"), P("dp", "tp"), rows),
                         check_vma=False)
```

```python
import functools

import jax
import jax.numpy as jnp
from jax import lax
from jax.experimental import pallas as pl
from jax.experimental.pallas import tpu as pltpu
from jax.sharding import PartitionSpec as P

MESH = pl.DeviceIdType.MESH
F32 = jnp.float32
BF16 = jnp.bfloat16
CORES = 2
PIECES = 4
NT = (((1,), (1,)), ((), ()))


def _silu_and_grad(u):
    s = jax.nn.sigmoid(u)
    return u * s, s * (1.0 + u * (1.0 - s))


def _main_kernel(nz, rows, x_hbm, dy_hbm, wg_hbm, wu_hbm, wd_hbm,
                 dx_ref, xg, dug, dwu_ref, dwd_ref,
                 dyg, duu, zz, zt, wg, wu, wd, wgt, wut, wdt,
                 pown, psend, psib, own_sum, own_send, own_sib, rsend, rrecv, fin,
                 own_sem, w_sem, ag_send, ag_recv, sib_send, sib_recv, ps_send, ps_recv, os_send, os_recv,
                 rs_send, rs_recv, fin_send, fin_recv):
    far = nz // 2
    near = nz - 1 - far
    me = lax.axis_index("tp")
    z = me // CORES
    c = lax.rem(me, CORES)
    width = x_hbm.shape[1]
    pw = width // PIECES
    blk = CORES * rows
    arrays = (xg, dyg)

    def dev(step, core):
        return {"tp": lax.rem(z + step + nz, nz) * CORES + core}

    def slot(off):
        return lax.rem(off + 2 * nz, nz)

    def step_of(d):
        return 1 if d == 0 else -1

    own = [pltpu.make_async_copy(src, dst.at[0, c], own_sem.at[i])
           for i, (src, dst) in enumerate(((x_hbm, xg), (dy_hbm, dyg)))]
    wcopies = [pltpu.make_async_copy(src, dst, w_sem.at[i])
               for i, (src, dst) in enumerate(((wg_hbm, wg), (wu_hbm, wu), (wd_hbm, wd)))]
    for cp in own:
        cp.start()
    barrier = pltpu.get_barrier_semaphore()
    peers = [dev(0, 1 - c), dev(1, c), dev(-1, c), dev(1, 1 - c), dev(-1, 1 - c)]
    for peer in peers:
        pl.semaphore_signal(barrier, inc=1, device_id=peer, device_id_type=MESH)
    pl.semaphore_wait(barrier, len(peers))

    def ag_copy(a, d, s):
        off = 1 - s if d == 0 else s - 1
        return pltpu.make_async_remote_copy(
            arrays[a].at[slot(off), c], arrays[a].at[slot(off - step_of(d)), c],
            ag_send.at[a, d, s - 1], ag_recv.at[a, d, s - 1], device_id=dev(step_of(d), c), device_id_type=MESH)

    def far_copy(a, d):
        off = 1 - far if d == 0 else far - 1
        cols = pl.ds(d * (width // 2), width // 2)
        return pltpu.make_async_remote_copy(
            arrays[a].at[slot(off), c, :, cols], arrays[a].at[far, c, :, cols],
            ag_send.at[a, d, far - 1], ag_recv.at[a, d, far - 1], device_id=dev(step_of(d), c), device_id_type=MESH)

    def sib_copy(a, o):
        return pltpu.make_async_remote_copy(
            arrays[a].at[o, c], arrays[a].at[o, c], sib_send.at[a, o], sib_recv.at[a, o],
            device_id=dev(0, 1 - c), device_id_type=MESH)

    def sib_wait(a, o):
        pltpu.make_async_remote_copy(
            arrays[a].at[o, 1 - c], arrays[a].at[o, 1 - c], sib_send.at[a, o], sib_recv.at[a, o],
            device_id=dev(0, 1 - c), device_id_type=MESH).wait_recv()

    FAR = "far"

    def kept(o, q):
        if o is FAR:
            return (far if q % 2 == 0 else 0), q // 2
        return o, q // 2

    def psum_copy(o, q):
        k = kept(o, q)
        return pltpu.make_async_remote_copy(
            psend.at[k], psib.at[k], ps_send.at[k], ps_recv.at[k], device_id=dev(0, 1 - c), device_id_type=MESH)

    def own_copy(q):
        return pltpu.make_async_remote_copy(
            own_send.at[q], own_sib.at[q], os_send.at[q], os_recv.at[q], device_id=dev(0, 1 - c), device_id_type=MESH)

    def stack(ref, offs):
        parts = [ref[o].reshape(blk, ref.shape[-1]) for o in offs]
        return parts[0] if len(parts) == 1 else jnp.concatenate(parts, axis=0)

    def unstack(ref, offs, v):
        for i, o in enumerate(offs):
            ref[o] = v[i * blk:(i + 1) * blk]

    def distinct(offs):
        return offs[:1] if offs[0] is offs[-1] else offs

    def x_part(offs):
        for o in distinct(offs):
            sib_wait(0, o)
        xb = stack(xg, offs)
        unstack(dug, offs, jnp.dot(xb, wg[...], preferred_element_type=F32).astype(BF16))
        unstack(duu, offs, jnp.dot(xb, wu[...], preferred_element_type=F32).astype(BF16))

    def y_part(offs, kind):
        for o in distinct(offs):
            sib_wait(1, o)
        g = jnp.dot(stack(dyg, offs), wdt[...], preferred_element_type=F32)
        ug = stack(dug, offs).astype(F32)
        uu = stack(duu, offs).astype(F32)
        a, da = _silu_and_grad(ug)
        unstack(zz, offs, (a * uu).astype(BF16))
        u = (g * a).astype(BF16)
        v = (g * uu * da).astype(BF16)
        unstack(duu, offs, u)
        unstack(dug, offs, v)
        for q in range(PIECES):
            cols = slice(q * pw, (q + 1) * pw)
            p = (jnp.dot(v, wgt[:, cols], preferred_element_type=F32)
                 + jnp.dot(u, wut[:, cols], preferred_element_type=F32))
            if kind == "own":
                own_sum[q] = jnp.where(c == 0, p[:rows], p[rows:])
                own_send[q] = jnp.where(c == 0, p[rows:], p[:rows]).astype(BF16)
                own_copy(q).start()
            elif kind == "far":
                pown[kept(FAR, q)] = p[:blk]
                psend[kept(FAR, q)] = p[:blk].astype(BF16)

                @pl.when(c == 0)
                def _():
                    psum_copy(FAR, q).start()
            else:
                first = c if q % 2 == 0 else 1 - c
                keep_o = offs[1] + first * (offs[0] - offs[1])
                send_o = offs[0] + offs[1] - keep_o
                pown[kept(keep_o, q)] = jnp.where(first == 1, p[:blk], p[blk:])
                psend[kept(send_o, q)] = jnp.where(first == 1, p[blk:], p[:blk]).astype(BF16)
                psum_copy(send_o, q).start()

    def hops(d, q):
        return far if (q + d) % 2 == 0 else near

    def rs_copy(d, q, s):
        k = (d, q // 2, s)
        return pltpu.make_async_remote_copy(
            rsend.at[k], rrecv.at[k], rs_send.at[k], rs_recv.at[k], device_id=dev(step_of(d), c), device_id_type=MESH)

    def fin_copy(d, q, h):
        return pltpu.make_async_remote_copy(
            rsend.at[d, q // 2, hops(d, q) - 1, pl.ds(h * rows, rows)], fin.at[d, q],
            fin_send.at[d, q // 2, h], fin_recv.at[d, q], device_id=dev(step_of(d), h), device_id_type=MESH)

    def rs_round(s, n):
        for q in range(PIECES):
            for d in range(2):
                if hops(d, q) != n:
                    continue
                o = (n - s if d == 0 else s - n) % nz
                o = FAR if o == far else o
                psum_copy(o, q).wait_recv()
                t = pown[kept(o, q)] + psib[kept(o, q)].astype(F32)
                if s > 0:
                    rs_copy(d, q, s - 1).wait_recv()
                    t = t + rrecv[d, q // 2, s - 1].astype(F32)
                rsend[d, q // 2, s] = t.astype(BF16)
                if s < n - 1:
                    rs_copy(d, q, s).start()
                else:
                    for h in range(CORES):
                        fin_copy(d, q, h).start()

    def rs_drain(n):
        for d in range(2):
            for q in range(PIECES):
                if hops(d, q) == n:
                    for s in range(n - 1):
                        rs_copy(d, q, s).wait_send()
                    for h in range(CORES):
                        fin_copy(d, q, h).wait_send()

    def grad_chunk(i, n):
        tok, w = nz * blk, width // n
        part = slice(i * w, (i + 1) * w)
        if i == 0:
            zt[...] = zz[...].reshape(tok, zz.shape[2]).T
        dwd_ref[:, part] = jnp.dot(zt[...], dyg[:, :, :, part].reshape(tok, w), preferred_element_type=F32)
        xt = xg[:, :, :, part].reshape(tok, w).T
        dwu_ref[part, :] = jnp.dot(xt, duu[...].reshape(tok, duu.shape[2]), preferred_element_type=F32)

    for a in range(2):
        own[a].wait()
        for d in range(2):
            ag_copy(a, d, 1).start()
        sib_copy(a, 0).start()
    for cp in wcopies:
        cp.start()
    for cp, w, wt in zip(wcopies, (wg, wu, wd), (wgt, wut, wdt)):
        cp.wait()
        wt[...] = w[...].T
    def event(a, s):
        for d in range(2):
            ag_copy(a, d, s).wait_recv()
            if isinstance(s, int):
                (ag_copy(a, d, s + 1) if s < near else far_copy(a, d)).start()
            else:
                @pl.when(s < near)
                def _():
                    ag_copy(a, d, s + 1).start()

                @pl.when(s == near)
                def _():
                    far_copy(a, d).start()
            sib_copy(a, nz - s if d == 0 else s).start()

    def far_event(a):
        for d in range(2):
            far_copy(a, d).wait_recv()
        sib_copy(a, far).start()

    x_part([0])
    event(0, 1)
    y_part([0], "own")
    event(1, 1)
    x_part([1, nz - 1])

    @pl.loop(2, near + 1)
    def _(s):
        event(0, s)
        y_part([s - 1, nz + 1 - s], "pair")
        event(1, s)
        x_part([s, nz - s])

    far_event(0)
    y_part([near, nz - near], "pair")
    far_event(1)

    x_part([far, far])

    @pl.when(c == 0)
    def _():
        rs_round(0, near)
    y_part([far, far], "far")

    @pl.when(c == 1)
    def _():
        for s in range(far):
            rs_round(s, far)
            if s < far - 1:
                grad_chunk(s, far - 1)
        rs_drain(far)

    @pl.when(c == 0)
    def _():
        for s in range(1, near):
            rs_round(s, near)
            grad_chunk(s - 1, near)
        grad_chunk(near - 1, near)
        rs_drain(near)

    for q in range(PIECES):
        own_copy(q).wait_recv()
        t = own_sum[q] + own_sib[q].astype(F32)
        for d in range(2):
            fin_copy(d, q, 0).wait_recv()
            t = t + fin[d, q].astype(F32)
        dx_ref[:, q * pw:(q + 1) * pw] = t.astype(BF16)

    for a in range(2):
        for d in range(2):
            for s in range(1, far):
                ag_copy(a, d, s).wait_send()
            far_copy(a, d).wait_send()
        for o in range(nz):
            sib_copy(a, o).wait_send()
    for q in range(PIECES):
        own_copy(q).wait_send()
    for o in range(1, nz):
        if o != far:
            for q in range(0, PIECES, 2):
                psum_copy(o, q).wait_send()

    @pl.when(c == 0)
    def _():
        for q in range(PIECES):
            psum_copy(FAR, q).wait_send()


def _grad_kernel(bw, x_ref, dug_ref, dx_vmem, dwu_vmem, dwd_vmem, dx_ref, dwg_ref, dwu_ref, dwd_ref, buf, done_sem, sem):
    steps = x_ref.shape[1] // bw
    stores = [pltpu.make_async_copy(src, dst, done_sem.at[i]) for i, (src, dst) in enumerate(
        ((dwd_vmem, dwd_ref), (dwu_vmem, dwu_ref), (dx_vmem, dx_ref)))]
    for cp in stores:
        cp.start()
    for i in range(steps):
        part = slice(i * bw, (i + 1) * bw)
        buf[part] = jnp.dot(x_ref[:, part].T, dug_ref[...], preferred_element_type=F32)
        stores.append(pltpu.make_async_copy(buf.at[part], dwg_ref.at[part], sem.at[i]))
        stores[-1].start()
    for cp in stores:
        cp.wait()


def solution(mesh):
    n = mesh.shape["tp"]
    nz = n // CORES

    def local(x, dy, wg, wu, wd):
        x, dy, wg, wu, wd = (pltpu.with_memory_space_constraint(v, pltpu.HBM) for v in (x, dy, wg, wu, wd))
        rows, width = x.shape
        hid = wg.shape[1]
        tok = rows * n
        far = nz // 2
        pw = width // PIECES
        S = jax.ShapeDtypeStruct
        hbm = pl.BlockSpec(memory_space=pltpu.HBM)
        dma = pltpu.SemaphoreType.DMA
        vmem = pl.BlockSpec(memory_space=pltpu.VMEM)
        dx, xg, dug, dwu, dwd = pl.pallas_call(
            functools.partial(_main_kernel, nz, rows),
            out_shape=[S((rows, width), BF16), S((nz, CORES, rows, width), BF16),
                       S((nz, CORES * rows, hid), BF16), S((width, hid), F32), S((hid, width), F32)],
            in_specs=[hbm] * 5,
            out_specs=[vmem] * 5,
            scratch_shapes=[
                pltpu.VMEM((nz, CORES, rows, width), BF16),
                pltpu.VMEM((nz, CORES * rows, hid), BF16),
                pltpu.VMEM((nz, CORES * rows, hid), BF16),
                pltpu.VMEM((hid, tok), BF16),
                pltpu.VMEM((width, hid), BF16),
                pltpu.VMEM((width, hid), BF16),
                pltpu.VMEM((hid, width), BF16),
                pltpu.VMEM((hid, width), BF16),
                pltpu.VMEM((hid, width), BF16),
                pltpu.VMEM((width, hid), BF16),
                pltpu.VMEM((nz, PIECES // 2, CORES * rows, pw), F32),
                pltpu.VMEM((nz, PIECES // 2, CORES * rows, pw), BF16),
                pltpu.VMEM((nz, PIECES // 2, CORES * rows, pw), BF16),
                pltpu.VMEM((PIECES, rows, pw), F32),
                pltpu.VMEM((PIECES, rows, pw), BF16),
                pltpu.VMEM((PIECES, rows, pw), BF16),
                pltpu.VMEM((2, PIECES // 2, far, CORES * rows, pw), BF16),
                pltpu.VMEM((2, PIECES // 2, far, CORES * rows, pw), BF16),
                pltpu.VMEM((2, PIECES, rows, pw), BF16),
                dma((2,)), dma((3,)),
                dma((2, 2, far)), dma((2, 2, far)),
                dma((2, nz)), dma((2, nz)),
                dma((nz, PIECES // 2)), dma((nz, PIECES // 2)),
                dma((PIECES,)), dma((PIECES,)),
                dma((2, PIECES // 2, far)), dma((2, PIECES // 2, far)),
                dma((2, PIECES // 2, CORES)), dma((2, PIECES)),
            ],
            compiler_params=pltpu.CompilerParams(
                collective_id=0, has_side_effects=True, vmem_limit_bytes=36 * 1024 * 1024),
            cost_estimate=pl.CostEstimate(
                flops=2 * 5 * tok * width * hid, bytes_accessed=6 * width * hid, transcendentals=tok * hid),
            name="gather_compute_scatter",
        )(x, dy, wg, wu, wd)
        bw = 1024
        dx, dwg, dwu, dwd = pl.pallas_call(
            functools.partial(_grad_kernel, bw),
            out_shape=[S((rows, width), BF16), S((width, hid), F32), S((width, hid), F32), S((hid, width), F32)],
            in_specs=[vmem] * 5,
            out_specs=[hbm] * 4,
            scratch_shapes=[pltpu.VMEM((width, hid), F32), dma((3,)), dma((width // bw,))],
            compiler_params=pltpu.CompilerParams(vmem_limit_bytes=16 * 1024 * 1024),
            cost_estimate=pl.CostEstimate(
                flops=2 * tok * width * hid, bytes_accessed=12 * width * hid, transcendentals=0),
            name="weight_grads",
        )(xg.reshape(tok, width), dug.reshape(tok, hid), dx, dwu, dwd)
        return dx, dwg, dwu, dwd

    rows = P(("dp", "tp"), None)
    return jax.shard_map(local, mesh=mesh,
                         in_specs=(rows, rows, P(None, "tp"), P(None, "tp"), P("tp", None)),
                         out_specs=(rows, P("dp", "tp"), P("dp", "tp"), rows),
                         check_vma=False)
```

```python
import functools

import jax
import jax.numpy as jnp
from jax import lax
from jax.experimental import pallas as pl
from jax.experimental.pallas import tpu as pltpu
from jax.sharding import PartitionSpec as P

MESH = pl.DeviceIdType.MESH
F32 = jnp.float32
BF16 = jnp.bfloat16
CORES = 2
PIECES = 4
NT = (((1,), (1,)), ((), ()))


def _silu_and_grad(u):
    s = jax.nn.sigmoid(u)
    return u * s, s * (1.0 + u * (1.0 - s))


def _main_kernel(nz, rows, x_hbm, dy_hbm, wg_hbm, wu_hbm, wd_hbm,
                 dx_ref, xg, dug, dwu_ref, dwd_ref,
                 dyg, duu, zz, zt, wg, wu, wd, wgt, wut, wdt,
                 pown, psend, psib, own_sum, own_send, own_sib, rsend, rrecv, fin,
                 own_sem, w_sem, ag_send, ag_recv, sib_send, sib_recv, ps_send, ps_recv, os_send, os_recv,
                 rs_send, rs_recv, fin_send, fin_recv):
    far = nz // 2
    near = nz - 1 - far
    me = lax.axis_index("tp")
    z = me // CORES
    c = lax.rem(me, CORES)
    width = x_hbm.shape[1]
    pw = width // PIECES
    blk = CORES * rows
    arrays = (xg, dyg)

    def dev(step, core):
        return {"tp": lax.rem(z + step + nz, nz) * CORES + core}

    def slot(off):
        return lax.rem(off + 2 * nz, nz)

    def step_of(d):
        return 1 if d == 0 else -1

    own = [pltpu.make_async_copy(src, dst.at[0, c], own_sem.at[i])
           for i, (src, dst) in enumerate(((x_hbm, xg), (dy_hbm, dyg)))]
    wcopies = [pltpu.make_async_copy(src, dst, w_sem.at[i])
               for i, (src, dst) in enumerate(((wg_hbm, wg), (wu_hbm, wu), (wd_hbm, wd)))]
    for cp in own:
        cp.start()
    barrier = pltpu.get_barrier_semaphore()
    peers = [dev(0, 1 - c), dev(1, c), dev(-1, c), dev(1, 1 - c), dev(-1, 1 - c)]
    for peer in peers:
        pl.semaphore_signal(barrier, inc=1, device_id=peer, device_id_type=MESH)
    pl.semaphore_wait(barrier, len(peers))

    def ag_copy(a, d, s):
        off = 1 - s if d == 0 else s - 1
        return pltpu.make_async_remote_copy(
            arrays[a].at[slot(off), c], arrays[a].at[slot(off - step_of(d)), c],
            ag_send.at[a, d, s - 1], ag_recv.at[a, d, s - 1], device_id=dev(step_of(d), c), device_id_type=MESH)

    def far_copy(a, d):
        off = 1 - far if d == 0 else far - 1
        cols = pl.ds(d * (width // 2), width // 2)
        return pltpu.make_async_remote_copy(
            arrays[a].at[slot(off), c, :, cols], arrays[a].at[far, c, :, cols],
            ag_send.at[a, d, far - 1], ag_recv.at[a, d, far - 1], device_id=dev(step_of(d), c), device_id_type=MESH)

    def sib_copy(a, o):
        return pltpu.make_async_remote_copy(
            arrays[a].at[o, c], arrays[a].at[o, c], sib_send.at[a, o], sib_recv.at[a, o],
            device_id=dev(0, 1 - c), device_id_type=MESH)

    def sib_wait(a, o):
        pltpu.make_async_remote_copy(
            arrays[a].at[o, 1 - c], arrays[a].at[o, 1 - c], sib_send.at[a, o], sib_recv.at[a, o],
            device_id=dev(0, 1 - c), device_id_type=MESH).wait_recv()

    FAR = "far"

    def kept(o, q):
        if o is FAR:
            return (far if q % 2 == 0 else 0), q // 2
        return o, q // 2

    def psum_copy(o, q):
        k = kept(o, q)
        return pltpu.make_async_remote_copy(
            psend.at[k], psib.at[k], ps_send.at[k], ps_recv.at[k], device_id=dev(0, 1 - c), device_id_type=MESH)

    def own_copy(q):
        return pltpu.make_async_remote_copy(
            own_send.at[q], own_sib.at[q], os_send.at[q], os_recv.at[q], device_id=dev(0, 1 - c), device_id_type=MESH)

    def stack(ref, offs):
        parts = [ref[o].reshape(blk, ref.shape[-1]) for o in offs]
        return parts[0] if len(parts) == 1 else jnp.concatenate(parts, axis=0)

    def unstack(ref, offs, v):
        for i, o in enumerate(offs):
            ref[o] = v[i * blk:(i + 1) * blk]

    def distinct(offs):
        return offs[:1] if offs[0] is offs[-1] else offs

    def x_part(offs):
        for o in distinct(offs):
            sib_wait(0, o)
        xb = stack(xg, offs)
        unstack(dug, offs, jnp.dot(xb, wg[...], preferred_element_type=F32).astype(BF16))
        unstack(duu, offs, jnp.dot(xb, wu[...], preferred_element_type=F32).astype(BF16))

    def y_part(offs, kind):
        for o in distinct(offs):
            sib_wait(1, o)
        g = jnp.dot(stack(dyg, offs), wdt[...], preferred_element_type=F32)
        ug = stack(dug, offs).astype(F32)
        uu = stack(duu, offs).astype(F32)
        a, da = _silu_and_grad(ug)
        unstack(zz, offs, (a * uu).astype(BF16))
        u = (g * a).astype(BF16)
        v = (g * uu * da).astype(BF16)
        unstack(duu, offs, u)
        unstack(dug, offs, v)
        for q in range(PIECES):
            cols = slice(q * pw, (q + 1) * pw)
            p = (jnp.dot(v, wgt[:, cols], preferred_element_type=F32)
                 + jnp.dot(u, wut[:, cols], preferred_element_type=F32))
            if kind == "own":
                own_sum[q] = jnp.where(c == 0, p[:rows], p[rows:])
                own_send[q] = jnp.where(c == 0, p[rows:], p[:rows]).astype(BF16)
                own_copy(q).start()
            elif kind == "far":
                pown[kept(FAR, q)] = p[:blk]
                psend[kept(FAR, q)] = p[:blk].astype(BF16)

                @pl.when(c == 0)
                def _():
                    psum_copy(FAR, q).start()

                if q > 0:
                    @pl.when(c == 1)
                    def _():
                        rs_message((q - 1) % 2, q - 1, 0, far)
            else:
                first = c if q % 2 == 0 else 1 - c
                keep_o = offs[1] + first * (offs[0] - offs[1])
                send_o = offs[0] + offs[1] - keep_o
                pown[kept(keep_o, q)] = jnp.where(first == 1, p[:blk], p[blk:])
                psend[kept(send_o, q)] = jnp.where(first == 1, p[blk:], p[:blk]).astype(BF16)
                psum_copy(send_o, q).start()

    def hops(d, q):
        return far if (q + d) % 2 == 0 else near

    def rs_copy(d, q, s):
        k = (d, q // 2, s)
        return pltpu.make_async_remote_copy(
            rsend.at[k], rrecv.at[k], rs_send.at[k], rs_recv.at[k], device_id=dev(step_of(d), c), device_id_type=MESH)

    def fin_copy(d, q, h):
        return pltpu.make_async_remote_copy(
            rsend.at[d, q // 2, hops(d, q) - 1, pl.ds(h * rows, rows)], fin.at[d, q],
            fin_send.at[d, q // 2, h], fin_recv.at[d, q], device_id=dev(step_of(d), h), device_id_type=MESH)

    def rs_message(d, q, s, n):
        o = (n - s if d == 0 else s - n) % nz
        o = FAR if o == far else o
        psum_copy(o, q).wait_recv()
        t = pown[kept(o, q)] + psib[kept(o, q)].astype(F32)
        if s > 0:
            rs_copy(d, q, s - 1).wait_recv()
            t = t + rrecv[d, q // 2, s - 1].astype(F32)
        rsend[d, q // 2, s] = t.astype(BF16)
        if s < n - 1:
            rs_copy(d, q, s).start()
        else:
            for h in range(CORES):
                fin_copy(d, q, h).start()

    def rs_round(s, n):
        for q in range(PIECES):
            for d in range(2):
                if hops(d, q) == n:
                    rs_message(d, q, s, n)

    def rs_drain(n):
        for d in range(2):
            for q in range(PIECES):
                if hops(d, q) == n:
                    for s in range(n - 1):
                        rs_copy(d, q, s).wait_send()
                    for h in range(CORES):
                        fin_copy(d, q, h).wait_send()

    def grad_chunk(i, n):
        tok, w = nz * blk, width // n
        part = slice(i * w, (i + 1) * w)
        if i == 0:
            zt[...] = zz[...].reshape(tok, zz.shape[2]).T
        dwd_ref[:, part] = jnp.dot(zt[...], dyg[:, :, :, part].reshape(tok, w), preferred_element_type=F32)
        xt = xg[:, :, :, part].reshape(tok, w).T
        dwu_ref[part, :] = jnp.dot(xt, duu[...].reshape(tok, duu.shape[2]), preferred_element_type=F32)

    for a in range(2):
        own[a].wait()
        for d in range(2):
            ag_copy(a, d, 1).start()
        sib_copy(a, 0).start()
    for cp in wcopies:
        cp.start()
    for cp, w, wt in zip(wcopies, (wg, wu, wd), (wgt, wut, wdt)):
        cp.wait()
        wt[...] = w[...].T
    def event(a, s):
        for d in range(2):
            ag_copy(a, d, s).wait_recv()
            if isinstance(s, int):
                (ag_copy(a, d, s + 1) if s < near else far_copy(a, d)).start()
            else:
                @pl.when(s < near)
                def _():
                    ag_copy(a, d, s + 1).start()

                @pl.when(s == near)
                def _():
                    far_copy(a, d).start()
            sib_copy(a, nz - s if d == 0 else s).start()

    def far_event(a):
        for d in range(2):
            far_copy(a, d).wait_recv()
        sib_copy(a, far).start()

    x_part([0])
    event(0, 1)
    y_part([0], "own")
    event(1, 1)
    x_part([1, nz - 1])

    @pl.loop(2, near + 1)
    def _(s):
        event(0, s)
        y_part([s - 1, nz + 1 - s], "pair")
        event(1, s)
        x_part([s, nz - s])

    far_event(0)
    y_part([near, nz - near], "pair")
    far_event(1)

    x_part([far, far])

    @pl.when(c == 0)
    def _():
        rs_round(0, near)
    y_part([far, far], "far")

    @pl.when(c == 1)
    def _():
        for s in range(far):
            if s > 0:
                rs_round(s, far)
            else:
                rs_message((PIECES - 1) % 2, PIECES - 1, 0, far)
            if s < far - 1:
                grad_chunk(s, far - 1)
        rs_drain(far)

    @pl.when(c == 0)
    def _():
        for s in range(1, near):
            rs_round(s, near)
            grad_chunk(s - 1, near)
        grad_chunk(near - 1, near)
        rs_drain(near)

    for q in range(PIECES):
        own_copy(q).wait_recv()
        t = own_sum[q] + own_sib[q].astype(F32)
        for d in range(2):
            fin_copy(d, q, 0).wait_recv()
            t = t + fin[d, q].astype(F32)
        dx_ref[:, q * pw:(q + 1) * pw] = t.astype(BF16)

    for a in range(2):
        for d in range(2):
            for s in range(1, far):
                ag_copy(a, d, s).wait_send()
            far_copy(a, d).wait_send()
        for o in range(nz):
            sib_copy(a, o).wait_send()
    for q in range(PIECES):
        own_copy(q).wait_send()
    for o in range(1, nz):
        if o != far:
            for q in range(0, PIECES, 2):
                psum_copy(o, q).wait_send()

    @pl.when(c == 0)
    def _():
        for q in range(PIECES):
            psum_copy(FAR, q).wait_send()


def _grad_kernel(bw, x_ref, dug_ref, dx_vmem, dwu_vmem, dwd_vmem, dx_ref, dwg_ref, dwu_ref, dwd_ref, buf, done_sem, sem):
    steps = x_ref.shape[1] // bw
    stores = [pltpu.make_async_copy(src, dst, done_sem.at[i]) for i, (src, dst) in enumerate(
        ((dwd_vmem, dwd_ref), (dwu_vmem, dwu_ref), (dx_vmem, dx_ref)))]
    for cp in stores:
        cp.start()
    for i in range(steps):
        part = slice(i * bw, (i + 1) * bw)
        buf[part] = jnp.dot(x_ref[:, part].T, dug_ref[...], preferred_element_type=F32)
        stores.append(pltpu.make_async_copy(buf.at[part], dwg_ref.at[part], sem.at[i]))
        stores[-1].start()
    for cp in stores:
        cp.wait()


def solution(mesh):
    n = mesh.shape["tp"]
    nz = n // CORES

    def local(x, dy, wg, wu, wd):
        x, dy, wg, wu, wd = (pltpu.with_memory_space_constraint(v, pltpu.HBM) for v in (x, dy, wg, wu, wd))
        rows, width = x.shape
        hid = wg.shape[1]
        tok = rows * n
        far = nz // 2
        pw = width // PIECES
        S = jax.ShapeDtypeStruct
        hbm = pl.BlockSpec(memory_space=pltpu.HBM)
        dma = pltpu.SemaphoreType.DMA
        vmem = pl.BlockSpec(memory_space=pltpu.VMEM)
        dx, xg, dug, dwu, dwd = pl.pallas_call(
            functools.partial(_main_kernel, nz, rows),
            out_shape=[S((rows, width), BF16), S((nz, CORES, rows, width), BF16),
                       S((nz, CORES * rows, hid), BF16), S((width, hid), F32), S((hid, width), F32)],
            in_specs=[hbm] * 5,
            out_specs=[vmem] * 5,
            scratch_shapes=[
                pltpu.VMEM((nz, CORES, rows, width), BF16),
                pltpu.VMEM((nz, CORES * rows, hid), BF16),
                pltpu.VMEM((nz, CORES * rows, hid), BF16),
                pltpu.VMEM((hid, tok), BF16),
                pltpu.VMEM((width, hid), BF16),
                pltpu.VMEM((width, hid), BF16),
                pltpu.VMEM((hid, width), BF16),
                pltpu.VMEM((hid, width), BF16),
                pltpu.VMEM((hid, width), BF16),
                pltpu.VMEM((width, hid), BF16),
                pltpu.VMEM((nz, PIECES // 2, CORES * rows, pw), F32),
                pltpu.VMEM((nz, PIECES // 2, CORES * rows, pw), BF16),
                pltpu.VMEM((nz, PIECES // 2, CORES * rows, pw), BF16),
                pltpu.VMEM((PIECES, rows, pw), F32),
                pltpu.VMEM((PIECES, rows, pw), BF16),
                pltpu.VMEM((PIECES, rows, pw), BF16),
                pltpu.VMEM((2, PIECES // 2, far, CORES * rows, pw), BF16),
                pltpu.VMEM((2, PIECES // 2, far, CORES * rows, pw), BF16),
                pltpu.VMEM((2, PIECES, rows, pw), BF16),
                dma((2,)), dma((3,)),
                dma((2, 2, far)), dma((2, 2, far)),
                dma((2, nz)), dma((2, nz)),
                dma((nz, PIECES // 2)), dma((nz, PIECES // 2)),
                dma((PIECES,)), dma((PIECES,)),
                dma((2, PIECES // 2, far)), dma((2, PIECES // 2, far)),
                dma((2, PIECES // 2, CORES)), dma((2, PIECES)),
            ],
            compiler_params=pltpu.CompilerParams(
                collective_id=0, has_side_effects=True, vmem_limit_bytes=36 * 1024 * 1024),
            cost_estimate=pl.CostEstimate(
                flops=2 * 5 * tok * width * hid, bytes_accessed=6 * width * hid, transcendentals=tok * hid),
            name="gather_compute_scatter",
        )(x, dy, wg, wu, wd)
        bw = 1024
        dx, dwg, dwu, dwd = pl.pallas_call(
            functools.partial(_grad_kernel, bw),
            out_shape=[S((rows, width), BF16), S((width, hid), F32), S((width, hid), F32), S((hid, width), F32)],
            in_specs=[vmem] * 5,
            out_specs=[hbm] * 4,
            scratch_shapes=[pltpu.VMEM((width, hid), F32), dma((3,)), dma((width // bw,))],
            compiler_params=pltpu.CompilerParams(vmem_limit_bytes=16 * 1024 * 1024),
            cost_estimate=pl.CostEstimate(
                flops=2 * tok * width * hid, bytes_accessed=12 * width * hid, transcendentals=0),
            name="weight_grads",
        )(xg.reshape(tok, width), dug.reshape(tok, hid), dx, dwu, dwd)
        return dx, dwg, dwu, dwd

    rows = P(("dp", "tp"), None)
    return jax.shard_map(local, mesh=mesh,
                         in_specs=(rows, rows, P(None, "tp"), P(None, "tp"), P("tp", None)),
                         out_specs=(rows, P("dp", "tp"), P("dp", "tp"), rows),
                         check_vma=False)
```
